32 devices in a mesh: pb: 8 (over y, x, core), ga: 4 (over z).
Axes of the slice: x: 2, y: 2, z: 4, core: 2. Of those that a mesh axis runs over, the one named last changes fastest.
Arguments:
- query_points: float32 [3, 32768], P(None, 'pb'), may hold values from 0 to 1
- cotangent: bfloat16 [64, 32768], P(None, 'pb'), may hold values from -6 to 6
- slab_ids: int32 [8, 32768], P(None, 'pb'), may hold values from -1 to 3
- rel_cells: int32 [8, 32768], P(None, 'pb'), may hold values from 0 to 511
- offsets: int32 [4, 256], P('ga', 'pb'), may hold values from 0 to 15872
- latent: bfloat16 [4, 64, 16384], P('ga', None, 'pb'), may hold values from -6 to 6
- w_in: float32 [80, 6], replicated, may hold values from -2.5 to 2.5
- b_in: float32 [80], replicated, may hold values from -3 to 3
- w_out: bfloat16 [64, 80], replicated, may hold values from -0.625 to 0.625
- b_out: float32 [64], replicated, may hold values from -3 to 3
Outputs:
- grid_grad: float32 [4, 64, 16384], P('ga', None, 'pb')
- w_in_grad: float32 [80, 6], replicated
- b_in_grad: float32 [80], replicated
- w_out_grad: float32 [64, 80], replicated
- b_out_grad: float32 [64], replicated
The draws below stay inside these ranges and needn't reach their ends.
Inputs may be any that keep to these rules, and one draw needn't show every extreme that they name: `slab_ids`: -1 marks a padding slot; otherwise the slab that holds the neighbour cell.
All inputs are finite; a program needn't handle non-finite values.
Results may differ from the reference program's by a relative error of at most 0.0085.
Values may be sent and summed in bfloat16 or wider, within the bound.
A program may use at most 64 MiB of HBM per device.

```python
import math
import jax
import jax.numpy as jnp
from jax import lax

CH = 64
HID = 80
KN = 8
TILE = 128
WIN = 512
GX = 64
ZS = 4
SLAB_CELLS = 16384
QUERIES = 32768
TILES = 256
N_GA = 4


def with_ends(array, rng, low, high):
    extent = array.shape
    spot = [jax.random.randint(jax.random.fold_in(rng, axis), (), 0, extent[axis]) for axis in range(len(extent))]
    array = array.at[tuple(spot)].set(low)
    longest = extent.index(max(extent))
    spot[longest] = (spot[longest] + 1) % extent[longest]
    return array.at[tuple(spot)].set(high)


def block_levels(rng, extent, split, least, top_value):
    loudness = 1.0
    for dim, blocks in split:
        draws = jax.random.uniform(jax.random.fold_in(jax.random.fold_in(rng, 6), dim), (blocks,), jnp.float32, least / len(split), top_value / len(split))
        loudness = loudness * jnp.repeat(jnp.exp(draws), extent[dim] // blocks).reshape((-1,) + (1,) * (len(extent) - 1 - dim))
    return loudness


def gaussian(rng, shape, deviation, bound, cuts=(), kind=jnp.bfloat16):
    drawn = jax.random.normal(rng, shape, jnp.float32) * deviation
    if len(cuts) > 0:
        drawn = block_levels(rng, shape, cuts, -0.22, 0.18) * drawn
    return jnp.clip(drawn, min=-bound, max=bound).astype(kind)


def setup_inputs(seed: int = 0) -> dict:
    key_list = jax.random.split(jax.random.key(seed), 11)
    return {
        "query_points": jnp.clip(1.0 * jax.random.uniform(key_list[0], (3, QUERIES), jnp.float32) ** block_levels(key_list[0], (3, QUERIES), ((1, 8),), -0.2, 0.2), 0.0, 1.0),
        "cotangent": gaussian(key_list[1], (CH, QUERIES), 1.0, 6.0, ((1, 8),)),
        "slab_ids": with_ends(jax.random.randint(key_list[2], (KN, QUERIES), -1, N_GA), jax.random.fold_in(key_list[2], 1), -1, N_GA - 1).astype(jnp.int32),
        "rel_cells": with_ends(jax.random.randint(key_list[3], (KN, QUERIES), 0, WIN), jax.random.fold_in(key_list[3], 1), 0, WIN - 1).astype(jnp.int32),
        "offsets": with_ends(jax.random.randint(key_list[4], (N_GA, TILES), 0, SLAB_CELLS - WIN + 1), jax.random.fold_in(key_list[4], 1), 0, SLAB_CELLS - WIN).astype(jnp.int32),
        "latent": gaussian(key_list[5], (N_GA, CH, SLAB_CELLS), 1.0, 6.0, ((0, 4), (2, 8))),
        "w_in": gaussian(key_list[6], (HID, 6), 6 ** -0.5, 2.5, (), jnp.float32),
        "b_in": gaussian(key_list[7], (HID,), 0.5, 3.0, (), jnp.float32),
        "w_out": gaussian(key_list[8], (CH, HID), HID ** -0.5, 0.625),
        "b_out": gaussian(key_list[9], (CH,), 0.5, 3.0, (), jnp.float32),
    }


def gelu_exact(values):
    return jax.nn.gelu(values, approximate=False)

def cell_centres(cell, slab):
    along_x = cell // (GX * ZS)
    along_y = cell // ZS % GX
    along_z = cell % ZS + slab * ZS
    return jnp.stack([(along_x.astype(jnp.float32) + 0.5) / GX, (along_y.astype(jnp.float32) + 0.5) / GX, (along_z.astype(jnp.float32) + 0.5) / GX], 0)

def reference(query_points, cotangent, slab_ids, rel_cells, offsets, latent, w_in, b_in, w_out, b_out):
    cells_slab = GX * GX * ZS
    latent_flat = jnp.transpose(latent, (1, 0, 2)).reshape(CH, N_GA * cells_slab)
    per_block = TILE * math.gcd(TILES, 64)
    count = QUERIES // per_block

    def reshape_blocks(values):
        return values.reshape(values.shape[0], count, per_block).transpose(1, 0, 2)

    def advance(running, inputs_block):
        grid_sum, totals = running
        number, points, cot_cols, slabs, rels = inputs_block
        tile_ids = (number * per_block + jnp.arange(per_block, dtype=jnp.int32)) // TILE
        slab_safe = jnp.maximum(slabs, 0)
        cell = offsets[slab_safe, tile_ids[None, :]] + rels
        flat_index = (slab_safe * cells_slab + cell).reshape(-1).astype(jnp.int32)
        mask_flat = (slabs >= 0).reshape(-1).astype(jnp.float32)
        centres = cell_centres(cell.reshape(-1), slab_safe.reshape(-1))
        features_in = jnp.concatenate([jnp.tile(points, (1, KN)), centres], 0)
        cot_flat = jnp.tile(cot_cols.astype(jnp.float32), (1, KN))
        feats = jnp.take(latent_flat, flat_index, axis=1).astype(jnp.float32)
        preact = jnp.dot(w_in, features_in, precision=lax.Precision.HIGHEST, preferred_element_type=jnp.float32) + b_in[:, None]
        hidden = gelu_exact(preact).astype(jnp.bfloat16)
        kernel = jnp.dot(w_out, hidden, preferred_element_type=jnp.float32) + b_out[:, None]
        grad_cell = (kernel * cot_flat * mask_flat).astype(jnp.bfloat16)
        grad_kernel = (feats * cot_flat * mask_flat).astype(jnp.bfloat16)
        grid_sum = grid_sum.at[:, flat_index].add(grad_cell.astype(jnp.float32))
        grad_w_out = lax.dot_general(grad_kernel, hidden, (((1,), (1,)), ((), ())), preferred_element_type=jnp.float32)
        grad_b_out = lax.optimization_barrier(jnp.sum(grad_kernel.astype(jnp.float32), 1))
        grad_hidden = lax.dot_general(w_out, grad_kernel, (((0,), (0,)), ((), ())), preferred_element_type=jnp.float32)
        grad_pre = jax.vjp(gelu_exact, preact)[1](grad_hidden)[0]
        grad_w_in = lax.dot_general(grad_pre, features_in, (((1,), (1,)), ((), ())), precision=lax.Precision.HIGHEST, preferred_element_type=jnp.float32)
        grad_b_in = lax.optimization_barrier(jnp.sum(grad_pre, 1))
        parts = (grad_w_in, grad_b_in, grad_w_out, grad_b_out)
        totals = tuple((old + new for old, new in zip(totals, parts)))
        return ((grid_sum, totals), None)
    start_totals = (jnp.zeros((HID, 6), jnp.float32), jnp.zeros((HID,), jnp.float32), jnp.zeros((CH, HID), jnp.float32), jnp.zeros((CH,), jnp.float32))
    start_grid = jnp.zeros((CH, N_GA * cells_slab), jnp.float32)
    inputs_all = (jnp.arange(count, dtype=jnp.int32), reshape_blocks(query_points), reshape_blocks(cotangent), reshape_blocks(slab_ids), reshape_blocks(rel_cells))
    (grid_sum, totals), _ = lax.scan(advance, (start_grid, start_totals), inputs_all)
    scale = float(QUERIES) ** (-0.5)
    grid_grad = grid_sum.reshape(CH, N_GA, cells_slab).transpose(1, 0, 2)
    return (grid_grad, totals[0] * scale, totals[1] * scale, totals[2] * scale, totals[3] * scale)
```

```python
import functools
import math

import jax
import jax.numpy as jnp
from jax import lax
from jax.experimental import pallas as pl
from jax.experimental.pallas import tpu as pltpu
from jax.sharding import PartitionSpec as P

KN = 8
TILE = 128
WIN = 512
GX = 64
ZS = 4
SPAN = WIN + 128
CAP = 256
EXTRA = 16
F32 = jnp.float32
BF16 = jnp.bfloat16


def dot(a, b):
    return jnp.dot(a, b, preferred_element_type=F32)


def dot_nt(a, b):
    return lax.dot_general(a, b, (((1,), (1,)), ((), ())), preferred_element_type=F32)


def window_base(offset, cells):
    return jnp.minimum(offset // 128 * 128, cells - SPAN)


def gelu_parts(x):
    z = jnp.abs(x) * (2.0**-0.5)
    t = 1.0 / (1.0 + 0.3275911 * z)
    e = jnp.exp(-0.5 * x * x)
    poly = ((((1.061405429 * t - 1.453152027) * t + 1.421413741) * t - 0.284496736) * t + 0.254829592) * t
    tail = 0.5 * poly * e
    cdf = jnp.where(x < 0, tail, 1.0 - tail)
    return x * cdf, cdf + x * e * ((2.0 * math.pi) ** -0.5)


def prepare(tiles, cells, meta_ref, ids_ref, rel_ref, pos_ref, relp_ref):
    slab = meta_ref[tiles]
    lives = []
    for t in range(tiles):
        cols = slice(t * TILE, (t + 1) * TILE)
        lives.append(jnp.where(ids_ref[:, cols] == slab, 1.0, 0.0))
        shift = meta_ref[t] - window_base(meta_ref[t], cells) + 1
        relp_ref[t * KN : (t + 1) * KN, :] = (rel_ref[:, cols] + shift).astype(F32)
    live = jnp.concatenate(lives, 0)
    rows = tiles * KN
    packed = live.astype(BF16)
    tri = jnp.where(
        lax.broadcasted_iota(jnp.int32, (TILE, TILE), 0) < lax.broadcasted_iota(jnp.int32, (TILE, TILE), 1), 1.0, 0.0
    ).astype(BF16)
    before = dot(packed, tri)
    total = dot(packed, jnp.ones((TILE, TILE), BF16))
    r = lax.broadcasted_iota(jnp.int32, (rows, rows), 0)
    c = lax.broadcasted_iota(jnp.int32, (rows, rows), 1)
    low = jnp.where((r // KN == c // KN) & (c < r), 1.0, 0.0).astype(BF16)
    start = dot(low, total.astype(BF16))
    pos_ref[...] = jnp.where(live > 0, before + start, -1.0e6)
    most = jnp.max(start + total).astype(jnp.int32)
    return (most + CAP - 1) // CAP


def pack_tile(t, c, base, slab, data_ref, pos_ref, relp_ref):
    channels = data_ref.shape[0] - EXTRA
    rows = pl.ds(pl.multiple_of(t * KN, KN), KN)
    pos = pos_ref[rows, :] - (c * CAP).astype(F32)
    relp = relp_ref[rows, :]
    place = lax.broadcasted_iota(jnp.int32, (CAP, TILE), 0).astype(F32)
    found = jnp.zeros((CAP, TILE), F32)
    for k in range(KN):
        found = jnp.where(pos[k : k + 1, :] == place, relp[k : k + 1, :], found)
    high = found.astype(BF16)
    low = (found - high.astype(F32)).astype(BF16)
    pick = jnp.where(found > 0, 1.0, 0.0).astype(BF16)
    drawn = dot_nt(data_ref[:, pl.ds(pl.multiple_of(t * TILE, TILE), TILE)], pick)
    ones = jnp.ones((8, TILE), BF16)
    spot = (dot_nt(ones, high) + dot_nt(ones, low)).astype(jnp.int32) - 1
    cell = spot + base
    along = [cell // (GX * ZS), cell // ZS % GX, cell % ZS + slab * ZS]
    along = [(a.astype(F32) + 0.5) / GX for a in along]
    row = lax.broadcasted_iota(jnp.int32, (8, CAP), 0)
    centre = jnp.where(row < 6, jnp.where(row % 3 == 0, along[0], jnp.where(row % 3 == 1, along[1], along[2])), 0.0)
    centre = jnp.concatenate([centre, jnp.zeros((8, CAP), F32)], 0)
    inputs = jnp.concatenate([drawn[channels:], centre], 0).astype(BF16)
    onehot = jnp.where(lax.broadcasted_iota(jnp.int32, (SPAN, CAP), 0) == spot[:1, :], 1.0, 0.0).astype(BF16)
    return drawn[:channels], inputs, onehot


def forward_kernel(tiles, group, meta_ref, data_ref, ids_ref, rel_ref, w1_ref, w2_ref, out_ref, pos_ref, relp_ref, grid_ref):
    cells = grid_ref.shape[1]
    chunks = prepare(tiles, cells, meta_ref, ids_ref, rel_ref, pos_ref, relp_ref)
    slab = meta_ref[tiles]

    grid_ref[...] = jnp.zeros_like(grid_ref)

    def body(i, _):
        c, g = i // (tiles // group), i % (tiles // group)
        done = []
        for u in range(group):
            t = g * group + u
            base = window_base(meta_ref[t], cells)
            cot, inputs, onehot = pack_tile(t, c, base, slab, data_ref, pos_ref, relp_ref)
            hidden = gelu_parts(dot(w1_ref[...], inputs))[0].astype(BF16)
            kernel = dot(w2_ref[...], jnp.concatenate([hidden, inputs], 0))
            done.append((base, dot_nt((kernel * cot).astype(BF16), onehot)))
        for base, part in done:
            at = pl.ds(pl.multiple_of(base, 128), SPAN)
            grid_ref[:, at] += part
        return 0

    lax.fori_loop(0, chunks * (tiles // group), body, 0)
    owned = out_ref.shape[2]
    for p in range(out_ref.shape[0]):
        out_ref[p] = grid_ref[:, p * owned : (p + 1) * owned].astype(out_ref.dtype)


def backward_kernel(tiles, group, meta_ref, data_ref, ids_ref, rel_ref, w1_ref, w2t_ref, feats_ref, out_ref, pos_ref, relp_ref):
    cells = feats_ref.shape[1]
    chunks = prepare(tiles, cells, meta_ref, ids_ref, rel_ref, pos_ref, relp_ref)
    slab = meta_ref[tiles]

    out_ref[...] = jnp.zeros_like(out_ref)

    def body(i, _):
        c, g = i // (tiles // group), i % (tiles // group)
        sums = []
        for u in range(group):
            t = g * group + u
            base = window_base(meta_ref[t], cells)
            cot, inputs, onehot = pack_tile(t, c, base, slab, data_ref, pos_ref, relp_ref)
            hidden, slope = gelu_parts(dot(w1_ref[...], inputs))
            feats = dot(feats_ref[:, pl.ds(pl.multiple_of(base, 128), SPAN)], onehot)
            grad_kernel = (feats * cot).astype(BF16)
            grad_pre = (dot(w2t_ref[...], grad_kernel) * slope).astype(BF16)
            sums.append(
                dot_nt(
                    jnp.concatenate([grad_kernel, grad_pre], 0),
                    jnp.concatenate([hidden.astype(BF16), inputs], 0),
                )
            )
        out_ref[...] += functools.reduce(lambda a, b: a + b, sums)
        return 0

    lax.fori_loop(0, chunks * (tiles // group), body, 0)


def split(values, parts):
    pieces = []
    for _ in range(parts):
        piece = lax.reduce_precision(values, 8, 7)
        pieces.append(piece.astype(BF16))
        values = values - piece
    return pieces


def shards(query_points, cotangent, slab_ids, rel_cells, offsets, latent, w_in, b_in, w_out, b_out):
    n_pb = lax.axis_size("pb")
    channels, owned = latent.shape[1], latent.shape[2]
    hid = w_in.shape[0]
    queries_dev = query_points.shape[1]
    tiles = queries_dev // TILE
    group = math.gcd(tiles, 4)
    cells = owned * n_pb

    slab_feats = lax.all_gather(latent[0], "pb", axis=1, tiled=True)

    meta = jnp.concatenate([offsets[0], lax.axis_index("ga")[None].astype(jnp.int32)])
    p_hi, p_lo = split(query_points, 2)
    ones = jnp.ones((3, queries_dev), BF16)
    data = jnp.concatenate([cotangent, p_hi, p_lo, p_hi, ones, jnp.zeros((EXTRA - 12, queries_dev), BF16)], 0)
    w_hi, w_lo = split(w_in, 2)
    b_parts = jnp.stack(split(b_in, 3), 1)
    w1 = jnp.concatenate(
        [w_hi[:, :3], w_hi[:, :3], w_lo[:, :3], b_parts, jnp.zeros((hid, EXTRA - 12), BF16),
         w_hi[:, 3:], w_lo[:, 3:], jnp.zeros((hid, 10), BF16)], 1)
    bo_parts = jnp.stack(split(b_out, 3), 1)
    w2 = jnp.concatenate(
        [w_out, jnp.zeros((channels, 9), BF16), bo_parts, jnp.zeros((channels, EXTRA + 4), BF16)], 1)

    vmem = pl.BlockSpec(memory_space=pltpu.VMEM)
    smem = pl.BlockSpec(memory_space=pltpu.SMEM)
    scratch = [pltpu.VMEM((tiles * KN, TILE), F32), pltpu.VMEM((tiles * KN, TILE), F32)]
    partial_grad = pl.pallas_call(
        functools.partial(forward_kernel, tiles, group),
        out_shape=jax.ShapeDtypeStruct((n_pb, channels, owned), BF16),
        in_specs=[smem] + [vmem] * 5,
        out_specs=vmem,
        scratch_shapes=scratch + [pltpu.VMEM((channels, cells), F32)],
        cost_estimate=pl.CostEstimate(flops=10**10, bytes_accessed=10**7, transcendentals=0),
        compiler_params=pltpu.CompilerParams(vmem_limit_bytes=40 * 2**20),
        name="forward",
    )(meta, data, slab_ids, rel_cells, w1, w2)
    received = lax.psum_scatter(partial_grad, "pb", scatter_dimension=0, tiled=True)
    sums = pl.pallas_call(
        functools.partial(backward_kernel, tiles, group),
        out_shape=jax.ShapeDtypeStruct((channels + hid, hid + EXTRA + 16), F32),
        in_specs=[smem] + [vmem] * 6,
        out_specs=vmem,
        scratch_shapes=scratch,
        cost_estimate=pl.CostEstimate(flops=10**10, bytes_accessed=10**7, transcendentals=0),
        compiler_params=pltpu.CompilerParams(vmem_limit_bytes=40 * 2**20),
        name="backward",
    )(meta, data, slab_ids, rel_cells, w1, w_out.T, slab_feats)
    scale = float(queries_dev * n_pb) ** (-0.5)
    sums = lax.psum(sums, ("pb", "ga")) * scale
    low = sums[channels:, hid:]
    w_in_grad = jnp.concatenate([low[:, 0:3] + low[:, 3:6], low[:, EXTRA : EXTRA + 3]], 1)
    return (
        received.astype(F32),
        w_in_grad,
        low[:, 9],
        sums[:channels, :hid],
        sums[:channels, hid + 9],
    )


def solution(mesh):
    return jax.shard_map(
        shards,
        mesh=mesh,
        in_specs=(
            P(None, "pb"),
            P(None, "pb"),
            P(None, "pb"),
            P(None, "pb"),
            P("ga", "pb"),
            P("ga", None, "pb"),
            P(),
            P(),
            P(),
            P(),
        ),
        out_specs=(P("ga", None, "pb"), P(), P(), P(), P()),
        check_vma=False,
    )
```
